256 devices in a mesh: groups: 2 (over y), nodes: 128 (over z, x, core).
Axes of the slice: x: 4, y: 2, z: 16, core: 2. Of those that a mesh axis runs over, the one named last changes fastest.
The devices are a block of a 4x16x16 slice.
Arguments:
- grid: bfloat16 [32768, 512], P(('groups', 'nodes')), parts along dimension 0, may hold values from -6 to 6
- hidden: bfloat16 [65536, 512], P(('groups', 'nodes')), parts along dimension 0, may hold values from -6 to 6
- enc_nbr: int32 [32768, 32], P('nodes'), may hold values from 0 to 16383, as said below
- dec_nbr: int32 [16384, 3], P('nodes'), may hold values from 0 to 32767, as said below
- enc_qkv: bfloat16 [512, 1536], replicated, may hold values from -0.25 to 0.25
- enc_out: bfloat16 [512, 512], replicated, may hold values from -0.25 to 0.25
- proc_qkv: bfloat16 [512, 1536], replicated, may hold values from -0.25 to 0.25
- proc_out: bfloat16 [512, 512], replicated, may hold values from -0.25 to 0.25
- dec_qkv: bfloat16 [512, 1536], replicated, may hold values from -0.25 to 0.25
- dec_out: bfloat16 [512, 512], replicated, may hold values from -0.25 to 0.25
- mlp_in: bfloat16 [512, 2048], replicated, may hold values from -0.25 to 0.25
- mlp_out: bfloat16 [2048, 512], replicated, may hold values from -0.125 to 0.125
Outputs:
- grid_out: bfloat16 [32768, 512], P(('groups', 'nodes')), parts along dimension 0
- hidden_two: bfloat16 [65536, 512], P(('groups', 'nodes')), parts along dimension 0
The draws below stay inside these ranges and needn't reach their ends.
There are 2 independent parts, one for each index of `groups`. The reference program is written for one: setup_inputs(seed, part) draws one part's arguments, and reference() takes and returns one part's arrays. A program takes and returns all parts, laid end to end along the dimension named above; an argument that names none is the same for every part. Nothing has to cross between parts.
Inputs may be any that keep to these rules, and one draw needn't show every extreme that they name: `enc_nbr`: row i names grid nodes of regions r - 1 to r + 1 only, with r = i // 256, region r holding grid nodes r * 128 to (r + 1) * 128 - 1. `dec_nbr`: row i names hidden nodes of regions r - 1 to r + 1 only, with r = i // 128, region r holding hidden nodes r * 256 to (r + 1) * 256 - 1.
All inputs are finite; a program needn't handle non-finite values.
Results may differ from the reference program's by a relative error of at most 0.015.
Values may be sent and summed in bfloat16 or wider, within the bound.
No kernel may reach another device: no remote copies, remote signals or barrier semaphores. Data moves between devices by JAX's collectives and lax.ppermute only.
A program may use at most 64 MiB of HBM per device.

```python
import jax
import jax.numpy as jnp
from jax import lax

D = 512
HEADS = 16
FF = 2048
GRID_DEV = 128
HID_DEV = 256
WIN = 512
K_ENC = 32
K_DEC = 3
GRID = 16384
HIDDEN_SIZE = 32768
N_NODES = 128


def near_lists(key, row_total, row_block, target_block, slot_count):
    region = jnp.arange(row_total, dtype=jnp.int32) // row_block
    lower_edge = jnp.maximum(region - 1, 0) * target_block
    upper_edge = jnp.minimum(region + 2, N_NODES) * target_block
    drawn_bits = jax.random.randint(key, (row_total, slot_count), 0, 1 << 30, dtype=jnp.int32)
    return lower_edge[:, None] + drawn_bits % (upper_edge - lower_edge)[:, None]


def draw_enc_nbr(key, part):
    return near_lists(jax.random.fold_in(key, 11), HIDDEN_SIZE, HID_DEV, GRID_DEV, K_ENC)


def draw_dec_nbr(key, part):
    return near_lists(jax.random.fold_in(key, 23), GRID, GRID_DEV, HID_DEV, K_DEC)


def block_levels(stream_key, shape, cuts, least, top_value):
    gain = 1.0
    for dim, shards_of in cuts:
        heights = jax.random.uniform(jax.random.fold_in(jax.random.fold_in(stream_key, 6), dim), (shards_of,), jnp.float32, least / len(cuts), top_value / len(cuts))
        gain = gain * jnp.repeat(jnp.exp(heights), shape[dim] // shards_of).reshape((-1,) + (1,) * (len(shape) - 1 - dim))
    return gain


def bell_draw(key, extent, width, reach, cuts=(), kind=jnp.bfloat16):
    gain = block_levels(key, extent, cuts, -0.22, 0.18) if cuts else 1.0
    array = jax.random.normal(key, extent, jnp.float32) * width * gain
    return jnp.minimum(jnp.maximum(array, -reach), reach).astype(kind)


def setup_inputs(seed: int = 0, part: int = 0) -> dict:
    key_list = jax.random.split(jax.random.key(seed), 13)
    part_keys = jax.random.split(jax.random.fold_in(key_list[12], part), 13)
    return {
        "grid": bell_draw(part_keys[0], (GRID, D), 1.0, 6.0, ((0, 128),)),
        "hidden": bell_draw(part_keys[1], (HIDDEN_SIZE, D), 1.0, 6.0, ((0, 128),)),
        "enc_nbr": draw_enc_nbr(jax.random.fold_in(key_list[12], 71), part),
        "dec_nbr": draw_dec_nbr(jax.random.fold_in(key_list[12], 71), part),
        "enc_qkv": bell_draw(key_list[4], (D, 3 * D), D ** -0.5, 0.25),
        "enc_out": bell_draw(key_list[5], (D, D), D ** -0.5, 0.25),
        "proc_qkv": bell_draw(key_list[6], (D, 3 * D), D ** -0.5, 0.25),
        "proc_out": bell_draw(key_list[7], (D, D), D ** -0.5, 0.25),
        "dec_qkv": bell_draw(key_list[8], (D, 3 * D), D ** -0.5, 0.25),
        "dec_out": bell_draw(key_list[9], (D, D), D ** -0.5, 0.25),
        "mlp_in": bell_draw(key_list[10], (D, FF), D ** -0.5, 0.25),
        "mlp_out": bell_draw(key_list[11], (FF, D), FF ** -0.5, 0.125),
    }


EPSILON = 1e-05

def layer_norm(values):
    values = values.astype(jnp.float32)
    center = values - lax.optimization_barrier(jnp.mean(values, axis=-1, keepdims=True))
    spread = lax.optimization_barrier(jnp.mean(center * center, axis=-1, keepdims=True))
    return (center * lax.rsqrt(spread + EPSILON)).astype(jnp.bfloat16)

def neighbour_attend(queries, key_values):
    row_count = queries.shape[0]
    slot_count = key_values.shape[1]
    model_width = queries.shape[1]
    head_size = model_width // HEADS
    query_heads = queries.astype(jnp.float32).reshape(row_count, HEADS, head_size)
    key_heads = key_values[:, :, :model_width].astype(jnp.float32).reshape(row_count, slot_count, HEADS, head_size)
    value_heads = key_values[:, :, model_width:].astype(jnp.float32).reshape(row_count, slot_count, HEADS, head_size)
    scores = jnp.einsum('nhd,nkhd->nhk', query_heads, key_heads) / jnp.sqrt(jnp.float32(head_size))
    weights = jax.nn.softmax(scores, axis=-1)
    return jnp.einsum('nhk,nkhd->nhd', weights, value_heads).reshape(row_count, model_width)

def window_attend(queries, key_values):
    row_count = queries.shape[0]
    key_count = key_values.shape[0]
    model_width = queries.shape[1]
    head_size = model_width // HEADS
    query_heads = queries.astype(jnp.float32).reshape(row_count, HEADS, head_size)
    key_heads = key_values[:, :model_width].astype(jnp.float32).reshape(key_count, HEADS, head_size)
    value_heads = key_values[:, model_width:].astype(jnp.float32).reshape(key_count, HEADS, head_size)
    scores = jnp.einsum('nhd,whd->hnw', query_heads, key_heads) / jnp.sqrt(jnp.float32(head_size))
    weights = jax.nn.softmax(scores, axis=-1)
    return jnp.einsum('hnw,whd->nhd', weights, value_heads).reshape(row_count, model_width)

def product(left, right):
    return jnp.dot(left, right, preferred_element_type=jnp.float32)

def reference(grid, hidden, enc_nbr, dec_nbr, enc_qkv, enc_out, proc_qkv, proc_out, dec_qkv, dec_out, mlp_in, mlp_out):
    model_width = grid.shape[1]
    grid_normed = layer_norm(grid)
    enc_queries = product(layer_norm(hidden), enc_qkv[:, :model_width]).astype(jnp.bfloat16)
    enc_pairs = product(grid_normed, enc_qkv[:, model_width:]).astype(jnp.bfloat16)

    def encode_block(inputs):
        block_queries, block_lists = inputs
        return neighbour_attend(block_queries, enc_pairs[block_lists]).astype(jnp.bfloat16)
    hidden_blocks = HIDDEN_SIZE // HID_DEV
    enc_mix = lax.map(encode_block, (enc_queries.reshape(hidden_blocks, HID_DEV, model_width), enc_nbr.reshape(hidden_blocks, HID_DEV, K_ENC))).reshape(HIDDEN_SIZE, model_width)
    hidden_one = (hidden.astype(jnp.float32) + product(enc_mix, enc_out)).astype(jnp.bfloat16)
    proc_all = product(layer_norm(hidden_one), proc_qkv).astype(jnp.bfloat16)

    def process_window(window_rows):
        return window_attend(window_rows[:, :model_width], window_rows[:, model_width:]).astype(jnp.bfloat16)
    proc_mix = lax.map(process_window, proc_all.reshape(HIDDEN_SIZE // WIN, WIN, 3 * model_width)).reshape(HIDDEN_SIZE, model_width)
    hidden_two = (hidden_one.astype(jnp.float32) + product(proc_mix, proc_out)).astype(jnp.bfloat16)
    dec_pairs = product(layer_norm(hidden_two), dec_qkv[:, model_width:]).astype(jnp.bfloat16)
    dec_queries = product(grid_normed, dec_qkv[:, :model_width]).astype(jnp.bfloat16)

    def decode_block(inputs):
        block_queries, block_lists = inputs
        return neighbour_attend(block_queries, dec_pairs[block_lists]).astype(jnp.bfloat16)
    grid_blocks = GRID // GRID_DEV
    dec_mix = lax.map(decode_block, (dec_queries.reshape(grid_blocks, GRID_DEV, model_width), dec_nbr.reshape(grid_blocks, GRID_DEV, K_DEC))).reshape(GRID, model_width)
    grid_one = (grid.astype(jnp.float32) + product(dec_mix, dec_out)).astype(jnp.bfloat16)
    mlp_hidden = jax.nn.gelu(product(layer_norm(grid_one), mlp_in)).astype(jnp.bfloat16)
    grid_out = (grid_one.astype(jnp.float32) + product(mlp_hidden, mlp_out)).astype(jnp.bfloat16)
    return (grid_out, hidden_two)
```

```python
import jax
import jax.numpy as jnp
from jax import lax
from jax.experimental import pallas as pl
from jax.experimental.pallas import tpu as pltpu
from jax.sharding import PartitionSpec as P

HEADS = 16
LANES = 128
EPSILON = 1e-05
LOG2E = 1.4426950408889634
MASKED = -1e30
BF16 = jnp.bfloat16
F32 = jnp.float32


def layer_norm(values):
    values = values.astype(F32)
    center = values - jnp.mean(values, axis=-1, keepdims=True)
    spread = jnp.mean(center * center, axis=-1, keepdims=True)
    return (center * lax.rsqrt(spread + EPSILON)).astype(BF16)


def dot(left, right):
    return jnp.dot(left, right, preferred_element_type=F32)


def dot_nt(left, right):
    return lax.dot_general(left, right, (((1,), (1,)), ((), ())), preferred_element_type=F32)


def lane_head(shape, head_size):
    return lax.broadcasted_iota(jnp.int32, shape, 1) // head_size


def block_columns(lists, pos, odd, rows):
    local = lists - pos * rows
    block = jnp.where(local < 0, -1, jnp.where(local < rows, 0, 1))
    inside = local - block * rows
    block = jnp.where(odd == 1, -block, block)
    return inside + jnp.where(block < 0, 2, block) * rows


def attend(q_ref, kv_ref, mix_ref, bias_ref=None):
    width = q_ref.shape[1]
    head_size = width // HEADS
    keys = kv_ref.shape[0]
    heads = lane_head((keys, LANES), head_size)
    zero = jnp.zeros((keys, LANES), BF16)
    one = jnp.ones((keys, LANES), BF16)
    for t in range(width // LANES):
        lanes = slice(t * LANES, (t + 1) * LANES)
        queries = q_ref[:, lanes]
        key_tile = kv_ref[:, lanes]
        value_tile = kv_ref[:, width + t * LANES : width + (t + 1) * LANES]
        total = None
        for h in range(LANES // head_size):
            chosen = heads == h
            scores = dot_nt(queries, jnp.where(chosen, key_tile, zero))
            if bias_ref is not None:
                scores = scores + bias_ref[...]
            weights = jnp.exp2(scores - jnp.max(scores, axis=1, keepdims=True)).astype(BF16)
            values = jnp.concatenate(
                [jnp.where(chosen, value_tile, zero), jnp.where(chosen, one, zero)], axis=1
            )
            part = dot(weights, values)
            total = part if total is None else total + part
        mix_ref[:, lanes] = (total[:, :LANES] / total[:, LANES:]).astype(BF16)


def prepare_kernel(
    pos_ref, grid_ref, hidden_ref, enc_nbr_ref, enc_qkv_ref, dec_qkv_ref,
    queries_ref, pairs_ref, bias_ref, dec_queries_ref,
):
    width = grid_ref.shape[1]
    rows = grid_ref.shape[0]
    scale = LOG2E / (width // HEADS) ** 0.5
    normed = layer_norm(grid_ref[...])
    pairs_ref[...] = dot(normed, enc_qkv_ref[:, width:]).astype(BF16)
    dec_queries_ref[...] = dot(normed, dec_qkv_ref[:, :width]).astype(BF16)
    queries = dot(layer_norm(hidden_ref[...]), enc_qkv_ref[:, :width])
    queries_ref[...] = (queries * scale).astype(BF16)
    pos = pos_ref[0]
    columns = block_columns(enc_nbr_ref[...], pos, pos % 2, rows)
    places = lax.broadcasted_iota(jnp.int32, bias_ref.shape, 1)
    counts = jnp.zeros(bias_ref.shape, F32)
    for k in range(columns.shape[1]):
        counts = counts + jnp.where(columns[:, k : k + 1] == places, 1.0, 0.0)
    bias_ref[...] = jnp.where(counts > 0.0, jnp.log2(jnp.maximum(counts, 1.0)), MASKED)


def encode_kernel(
    queries_ref, pairs_ref, bias_ref, partner_ref, off_ref, hidden_ref, qkv_ref, out_ref,
    result_ref, pairs, mix,
):
    width = hidden_ref.shape[1]
    rows = pairs_ref.shape[0]
    pairs[:rows] = pairs_ref[...]
    normed = jnp.concatenate([layer_norm(partner_ref[...]), layer_norm(off_ref[...])], axis=0)
    pairs[rows:] = dot(normed, qkv_ref[:, width:]).astype(BF16)
    attend(queries_ref, pairs, mix, bias_ref)
    result_ref[...] = (hidden_ref[...].astype(F32) + dot(mix[...], out_ref[...])).astype(BF16)


def project_kernel(hidden_ref, qkv_ref, queries_ref, pairs_ref):
    width = hidden_ref.shape[1]
    scale = LOG2E / (width // HEADS) ** 0.5
    normed = layer_norm(hidden_ref[...])
    queries_ref[...] = (dot(normed, qkv_ref[:, :width]) * scale).astype(BF16)
    pairs_ref[...] = dot(normed, qkv_ref[:, width:]).astype(BF16)


def process_kernel(queries_ref, pairs_ref, hidden_ref, partner_ref, qkv_ref, out_ref, result_ref, pairs, mix):
    width = hidden_ref.shape[1]
    rows = hidden_ref.shape[0]
    pairs[:rows] = pairs_ref[...]
    pairs[rows:] = dot(layer_norm(partner_ref[...]), qkv_ref[:, width:]).astype(BF16)
    attend(queries_ref, pairs, mix)
    result_ref[...] = (hidden_ref[...].astype(F32) + dot(mix[...], out_ref[...])).astype(BF16)


def decode_kernel(
    pos_ref, own_ref, partner_ref, off_ref, nbr_ref, queries_ref, grid_ref, qkv_ref, out_ref,
    mlp_in_ref, mlp_out_ref, result_ref, normed,
):
    width = own_ref.shape[1]
    head_size = width // HEADS
    rows = own_ref.shape[0]
    grid_rows = grid_ref.shape[0]
    slots = nbr_ref.shape[1]
    scale = LOG2E / head_size**0.5
    normed[:rows] = layer_norm(own_ref[...])
    normed[rows : 2 * rows] = layer_norm(partner_ref[...])
    normed[2 * rows :] = layer_norm(off_ref[...])
    pos = pos_ref[0]
    columns = block_columns(nbr_ref[...], pos, pos % 2, rows)
    places = lax.broadcasted_iota(jnp.int32, (grid_rows, 3 * rows), 1)
    picks = jnp.concatenate(
        [jnp.where(columns[:, j : j + 1] == places, 1.0, 0.0).astype(BF16) for j in range(slots)],
        axis=0,
    )
    rows_picked = dot(picks, normed[...]).astype(BF16)
    pairs = dot(rows_picked, qkv_ref[:, width:]).astype(BF16)
    feature = lax.broadcasted_iota(jnp.int32, (width, LANES), 0) // head_size
    heads = lax.broadcasted_iota(jnp.int32, (width, LANES), 1)
    gather_heads = jnp.where(feature == heads, 1.0, 0.0).astype(BF16)
    queries = queries_ref[...].astype(F32)
    scores = []
    for j in range(slots):
        keys = pairs[j * grid_rows : (j + 1) * grid_rows, :width].astype(F32)
        scores.append(dot((queries * keys).astype(BF16), gather_heads) * scale)
    maxima = scores[0]
    for j in range(1, slots):
        maxima = jnp.maximum(maxima, scores[j])
    weights = [jnp.exp2(s - maxima) for s in scores]
    total = weights[0]
    for j in range(1, slots):
        total = total + weights[j]
    mix = None
    for j in range(slots):
        spread = dot_nt((weights[j] / total).astype(BF16), gather_heads)
        part = spread * pairs[j * grid_rows : (j + 1) * grid_rows, width:].astype(F32)
        mix = part if mix is None else mix + part
    grid_one = (grid_ref[...].astype(F32) + dot(mix.astype(BF16), out_ref[...])).astype(BF16)
    inner = jax.nn.gelu(dot(layer_norm(grid_one), mlp_in_ref[...])).astype(BF16)
    result_ref[...] = (grid_one.astype(F32) + dot(inner, mlp_out_ref[...])).astype(BF16)


def call(kernel, outs, scratch, flops, *args, scalars=0):
    vmem = pl.BlockSpec(memory_space=pltpu.VMEM)
    smem = pl.BlockSpec(memory_space=pltpu.SMEM)
    return pl.pallas_call(
        kernel,
        out_shape=[jax.ShapeDtypeStruct(shape, kind) for shape, kind in outs],
        in_specs=[smem] * scalars + [vmem] * (len(args) - scalars),
        out_specs=[vmem] * len(outs),
        scratch_shapes=[pltpu.VMEM(shape, kind) for shape, kind in scratch],
        cost_estimate=pl.CostEstimate(flops=flops, transcendentals=0, bytes_accessed=0),
        compiler_params=pltpu.CompilerParams(vmem_limit_bytes=48 << 20),
        name=kernel.__name__,
    )(*args)


def local(
    grid, hidden, enc_nbr, dec_nbr, enc_qkv, enc_out, proc_qkv, proc_out, dec_qkv, dec_out,
    mlp_in, mlp_out,
):
    grid_rows, width = grid.shape
    rows = hidden.shape[0]
    devices = lax.axis_size("nodes")
    pos = lax.axis_index("nodes").astype(jnp.int32).reshape(1)
    inner_pairs = [(i, i ^ 1) for i in range(devices)]
    outer_pairs = [(i, i + 1) for i in range(1, devices - 1, 2)]
    outer_pairs = outer_pairs + [(j, i) for i, j in outer_pairs]

    def exchange(shard):
        off = lax.ppermute(shard, "nodes", outer_pairs)
        return lax.ppermute(shard, "nodes", inner_pairs), off

    grid_partner, grid_off = exchange(grid)
    queries, pairs, bias, dec_queries = call(
        prepare_kernel,
        [
            ((rows, width), BF16),
            ((grid_rows, 2 * width), BF16),
            ((rows, 3 * grid_rows), F32),
            ((grid_rows, width), BF16),
        ],
        [],
        2_000_000_000,
        pos, grid, hidden, enc_nbr, enc_qkv, dec_qkv,
        scalars=1,
    )
    (hidden_one,) = call(
        encode_kernel,
        [((rows, width), BF16)],
        [((3 * grid_rows, 2 * width), BF16), ((rows, width), BF16)],
        4_000_000_000,
        queries, pairs, bias, grid_partner, grid_off, hidden, enc_qkv, enc_out,
    )
    one_partner = lax.ppermute(hidden_one, "nodes", inner_pairs)
    queries, pairs = call(
        project_kernel,
        [((rows, width), BF16), ((rows, 2 * width), BF16)],
        [],
        1_000_000_000,
        hidden_one, proc_qkv,
    )
    (hidden_two,) = call(
        process_kernel,
        [((rows, width), BF16)],
        [((2 * rows, 2 * width), BF16), ((rows, width), BF16)],
        4_000_000_000,
        queries, pairs, hidden_one, one_partner, proc_qkv, proc_out,
    )
    two_partner, two_off = exchange(hidden_two)
    (grid_out,) = call(
        decode_kernel,
        [((grid_rows, width), BF16)],
        [((3 * rows, width), BF16)],
        4_000_000_000,
        pos, hidden_two, two_partner, two_off, dec_nbr, dec_queries, grid, dec_qkv, dec_out,
        mlp_in, mlp_out,
        scalars=1,
    )
    return (grid_out, hidden_two)


def solution(mesh):
    part = P(("groups", "nodes"), None)
    nodes = P("nodes", None)
    return jax.shard_map(
        local,
        mesh=mesh,
        in_specs=(part, part, nodes, nodes) + (P(),) * 8,
        out_specs=(part, part),
        check_vma=False,
    )
```

```python
import jax
import jax.numpy as jnp
from jax import lax
from jax.experimental import pallas as pl
from jax.experimental.pallas import tpu as pltpu
from jax.sharding import PartitionSpec as P

HEADS = 16
LANES = 128
EPSILON = 1e-05
LOG2E = 1.4426950408889634
MASKED = -1e30
BF16 = jnp.bfloat16
F32 = jnp.float32


def layer_norm(values):
    values = values.astype(F32)
    center = values - jnp.mean(values, axis=-1, keepdims=True)
    spread = jnp.mean(center * center, axis=-1, keepdims=True)
    return (center * lax.rsqrt(spread + EPSILON)).astype(BF16)


def dot(left, right):
    return jnp.dot(left, right, preferred_element_type=F32)


def dot_nt(left, right):
    return lax.dot_general(left, right, (((1,), (1,)), ((), ())), preferred_element_type=F32)


def lane_head(shape, head_size):
    return lax.broadcasted_iota(jnp.int32, shape, 1) // head_size


def block_columns(lists, pos, odd, rows):
    local = lists - pos * rows
    block = jnp.where(local < 0, -1, jnp.where(local < rows, 0, 1))
    inside = local - block * rows
    block = jnp.where(odd == 1, -block, block)
    return inside + jnp.where(block < 0, 2, block) * rows


def attend(q_ref, kv_ref, mix_ref, bias_ref=None):
    width = q_ref.shape[1]
    head_size = width // HEADS
    keys = kv_ref.shape[0]
    heads = lane_head((keys, LANES), head_size)
    zero = jnp.zeros((keys, LANES), BF16)
    one = jnp.ones((keys, LANES), BF16)
    for t in range(width // LANES):
        lanes = slice(t * LANES, (t + 1) * LANES)
        queries = q_ref[:, lanes]
        key_tile = kv_ref[:, lanes]
        value_tile = kv_ref[:, width + t * LANES : width + (t + 1) * LANES]
        total = None
        for h in range(LANES // head_size):
            chosen = heads == h
            scores = dot_nt(queries, jnp.where(chosen, key_tile, zero))
            if bias_ref is not None:
                scores = scores + bias_ref[...]
            weights = jnp.exp2(scores - jnp.max(scores, axis=1, keepdims=True)).astype(BF16)
            values = jnp.concatenate(
                [jnp.where(chosen, value_tile, zero), jnp.where(chosen, one, zero)], axis=1
            )
            part = dot(weights, values)
            total = part if total is None else total + part
        mix_ref[:, lanes] = (total[:, :LANES] / total[:, LANES:]).astype(BF16)


def prepare_kernel(
    pos_ref, grid_hbm, hidden_hbm, enc_nbr_hbm, enc_qkv_hbm,
    queries_ref, pairs_ref, bias_ref,
    grid_ref, hidden_ref, enc_nbr_ref, enc_qkv_ref, arrived,
):
    width = grid_ref.shape[1]
    rows = grid_ref.shape[0]
    scale = LOG2E / (width // HEADS) ** 0.5
    copies = [
        pltpu.make_async_copy(source, target, arrived.at[i])
        for i, (source, target) in enumerate(
            [
                (enc_nbr_hbm, enc_nbr_ref),
                (grid_hbm, grid_ref),
                (hidden_hbm, hidden_ref),
                (enc_qkv_hbm, enc_qkv_ref),
            ]
        )
    ]
    for copy in copies:
        copy.start()
    copies[0].wait()
    pos = pos_ref[0]
    columns = block_columns(enc_nbr_ref[...], pos, pos % 2, rows)
    half = bias_ref.shape[1] // 2
    columns = (columns - half).astype(F32).astype(BF16)
    one = jnp.ones((rows, columns.shape[1]), BF16)
    for b in range(bias_ref.shape[1] // rows):
        places = b * rows - half + lax.broadcasted_iota(jnp.int32, one.shape, 0)
        places = places.astype(F32).astype(BF16)
        counts = jnp.zeros_like(one)
        for k in range(columns.shape[0]):
            counts = counts + jnp.where(columns[k : k + 1] == places, one, jnp.zeros_like(one))
        counts = counts.astype(F32)
        bias = jnp.where(counts > 0.0, jnp.log2(jnp.maximum(counts, 1.0)), MASKED)
        bias_ref[:, b * rows : (b + 1) * rows] = bias.T
    copies[1].wait()
    copies[2].wait()
    normed = layer_norm(grid_ref[...])
    normed_hidden = layer_norm(hidden_ref[...])
    copies[3].wait()
    pairs_ref[...] = dot(normed, enc_qkv_ref[:, width:]).astype(BF16)
    queries = dot(normed_hidden, enc_qkv_ref[:, :width])
    queries_ref[...] = (queries * scale).astype(BF16)


def encode_kernel(
    queries_ref, pairs_ref, bias_ref, partner_ref, off_ref, hidden_ref, qkv_ref, out_ref,
    result_ref, pairs, mix,
):
    width = hidden_ref.shape[1]
    rows = pairs_ref.shape[0]
    pairs[:rows] = pairs_ref[...]
    normed = jnp.concatenate([layer_norm(partner_ref[...]), layer_norm(off_ref[...])], axis=0)
    pairs[rows:] = dot(normed, qkv_ref[:, width:]).astype(BF16)
    attend(queries_ref, pairs, mix, bias_ref)
    result_ref[...] = (hidden_ref[...].astype(F32) + dot(mix[...], out_ref[...])).astype(BF16)


def project_kernel(hidden_ref, qkv_ref, queries_ref, pairs_ref):
    width = hidden_ref.shape[1]
    scale = LOG2E / (width // HEADS) ** 0.5
    normed = layer_norm(hidden_ref[...])
    queries_ref[...] = (dot(normed, qkv_ref[:, :width]) * scale).astype(BF16)
    pairs_ref[...] = dot(normed, qkv_ref[:, width:]).astype(BF16)


def process_kernel(queries_ref, pairs_ref, hidden_ref, partner_ref, qkv_ref, out_ref, result_ref, pairs, mix):
    width = hidden_ref.shape[1]
    rows = hidden_ref.shape[0]
    pairs[:rows] = pairs_ref[...]
    pairs[rows:] = dot(layer_norm(partner_ref[...]), qkv_ref[:, width:]).astype(BF16)
    attend(queries_ref, pairs, mix)
    result_ref[...] = (hidden_ref[...].astype(F32) + dot(mix[...], out_ref[...])).astype(BF16)


def picks_of(columns, first, rows):
    places = first + lax.broadcasted_iota(jnp.int32, (columns.shape[0], rows), 1)
    return jnp.concatenate(
        [
            jnp.where(columns[:, j : j + 1] == places, 1.0, 0.0).astype(BF16)
            for j in range(columns.shape[1])
        ],
        axis=0,
    )


def gather_kernel(
    pos_ref, own_ref, partner_ref, nbr_ref, grid_hbm, qkv_hbm,
    two_hbm, queries_ref, picked_ref, off_picks_ref, grid_ref,
    normed, qkv_ref, arrived, written,
):
    width = own_ref.shape[1]
    rows = own_ref.shape[0]
    grid_copy = pltpu.make_async_copy(grid_hbm, grid_ref, arrived.at[0])
    qkv_copy = pltpu.make_async_copy(qkv_hbm.at[:, :width], qkv_ref, arrived.at[1])
    copy = pltpu.make_async_copy(own_ref, two_hbm, written)
    grid_copy.start()
    qkv_copy.start()
    copy.start()
    pos = pos_ref[0]
    columns = block_columns(nbr_ref[...], pos, pos % 2, rows)
    off_picks_ref[...] = picks_of(columns, 2 * rows, rows)
    normed[:rows] = layer_norm(own_ref[...])
    normed[rows:] = layer_norm(partner_ref[...])
    picked_ref[...] = dot(picks_of(columns, 0, 2 * rows), normed[...]).astype(BF16)
    grid_copy.wait()
    qkv_copy.wait()
    queries_ref[...] = dot(layer_norm(grid_ref[...]), qkv_ref[...]).astype(BF16)
    copy.wait()


def decode_kernel(
    off_ref, off_picks_ref, picked_ref, queries_ref, grid_ref, qkv_ref, out_ref,
    mlp_in_ref, mlp_out_ref, result_ref,
):
    width = off_ref.shape[1]
    head_size = width // HEADS
    grid_rows = grid_ref.shape[0]
    slots = picked_ref.shape[0] // grid_rows
    scale = LOG2E / head_size**0.5
    rows_picked = picked_ref[...] + dot(off_picks_ref[...], layer_norm(off_ref[...])).astype(BF16)
    pairs = dot(rows_picked, qkv_ref[:, width:]).astype(BF16)
    feature = lax.broadcasted_iota(jnp.int32, (width, LANES), 0) // head_size
    heads = lax.broadcasted_iota(jnp.int32, (width, LANES), 1)
    gather_heads = jnp.where(feature == heads, 1.0, 0.0).astype(BF16)
    queries = queries_ref[...].astype(F32)
    scores = []
    for j in range(slots):
        keys = pairs[j * grid_rows : (j + 1) * grid_rows, :width].astype(F32)
        scores.append(dot((queries * keys).astype(BF16), gather_heads) * scale)
    maxima = scores[0]
    for j in range(1, slots):
        maxima = jnp.maximum(maxima, scores[j])
    weights = [jnp.exp2(s - maxima) for s in scores]
    total = weights[0]
    for j in range(1, slots):
        total = total + weights[j]
    mix = None
    for j in range(slots):
        spread = dot_nt((weights[j] / total).astype(BF16), gather_heads)
        part = spread * pairs[j * grid_rows : (j + 1) * grid_rows, width:].astype(F32)
        mix = part if mix is None else mix + part
    grid_one = (grid_ref[...].astype(F32) + dot(mix.astype(BF16), out_ref[...])).astype(BF16)
    inner = jax.nn.gelu(dot(layer_norm(grid_one), mlp_in_ref[...])).astype(BF16)
    result_ref[...] = (grid_one.astype(F32) + dot(inner, mlp_out_ref[...])).astype(BF16)


def call(kernel, outs, scratch, flops, limit, *args, scalars=0, anywhere=(), out_anywhere=()):
    vmem = pl.BlockSpec(memory_space=pltpu.VMEM)
    smem = pl.BlockSpec(memory_space=pltpu.SMEM)
    hbm = pl.BlockSpec(memory_space=pltpu.HBM)
    args = [
        pltpu.with_memory_space_constraint(x, pltpu.HBM) if i in anywhere else x
        for i, x in enumerate(args)
    ]
    return pl.pallas_call(
        kernel,
        out_shape=[jax.ShapeDtypeStruct(shape, kind) for shape, kind in outs],
        in_specs=[
            smem if i < scalars else hbm if i in anywhere else vmem for i in range(len(args))
        ],
        out_specs=[hbm if i in out_anywhere else vmem for i in range(len(outs))],
        scratch_shapes=scratch,
        cost_estimate=pl.CostEstimate(flops=flops, transcendentals=0, bytes_accessed=0),
        compiler_params=pltpu.CompilerParams(vmem_limit_bytes=limit << 20),
    )(*args)


def step(
    grid, hidden, enc_nbr, dec_nbr, enc_qkv, enc_out, proc_qkv, proc_out, dec_qkv, dec_out,
    mlp_in, mlp_out,
):
    grid_rows, width = grid.shape
    rows = hidden.shape[0]
    slots = dec_nbr.shape[1]
    devices = lax.axis_size("nodes")
    pos = lax.axis_index("nodes").astype(jnp.int32).reshape(1)
    inner_pairs = [(i, i ^ 1) for i in range(devices)]
    outer_pairs = [(i, i + 1) for i in range(1, devices - 1, 2)]
    outer_pairs = outer_pairs + [(j, i) for i, j in outer_pairs]

    def exchange(shard):
        off = lax.ppermute(shard, "nodes", outer_pairs)
        return lax.ppermute(shard, "nodes", inner_pairs), off

    grid_partner, grid_off = exchange(grid)
    queries, pairs, bias = call(
        prepare_kernel,
        [((rows, width), BF16), ((grid_rows, 2 * width), BF16), ((rows, 3 * grid_rows), F32)],
        [
            pltpu.VMEM(grid.shape, BF16),
            pltpu.VMEM(hidden.shape, BF16),
            pltpu.VMEM(enc_nbr.shape[::-1], jnp.int32),
            pltpu.VMEM(enc_qkv.shape, BF16),
            pltpu.SemaphoreType.DMA((4,)),
        ],
        2_000_000_000,
        16,
        pos, grid, hidden, enc_nbr.T, enc_qkv,
        scalars=1,
        anywhere=(1, 2, 3, 4),
    )
    (hidden_one,) = call(
        encode_kernel,
        [((rows, width), BF16)],
        [pltpu.VMEM((3 * grid_rows, 2 * width), BF16), pltpu.VMEM((rows, width), BF16)],
        4_000_000_000,
        16,
        queries, pairs, bias, grid_partner, grid_off, hidden, enc_qkv, enc_out,
    )
    one_partner = lax.ppermute(hidden_one, "nodes", inner_pairs)
    queries, pairs = call(
        project_kernel,
        [((rows, width), BF16), ((rows, 2 * width), BF16)],
        [],
        1_000_000_000,
        16,
        hidden_one, proc_qkv,
    )
    (two_near,) = call(
        process_kernel,
        [((rows, width), BF16)],
        [pltpu.VMEM((2 * rows, 2 * width), BF16), pltpu.VMEM((rows, width), BF16)],
        4_000_000_000,
        16,
        queries, pairs, hidden_one, one_partner, proc_qkv, proc_out,
    )
    two_partner, two_off = exchange(two_near)
    hidden_two, dec_queries, picked, off_picks, grid_near = call(
        gather_kernel,
        [
            ((rows, width), BF16),
            ((grid_rows, width), BF16),
            ((slots * grid_rows, width), BF16),
            ((slots * grid_rows, rows), BF16),
            ((grid_rows, width), BF16),
        ],
        [
            pltpu.VMEM((2 * rows, width), BF16),
            pltpu.VMEM((width, width), BF16),
            pltpu.SemaphoreType.DMA((2,)),
            pltpu.SemaphoreType.DMA,
        ],
        1_000_000_000,
        16,
        pos, two_near, two_partner, dec_nbr, grid, dec_qkv,
        scalars=1,
        anywhere=(4, 5),
        out_anywhere=(0,),
    )
    (grid_out,) = call(
        decode_kernel,
        [((grid_rows, width), BF16)],
        [],
        4_000_000_000,
        16,
        two_off, off_picks, picked, dec_queries, grid_near, dec_qkv, dec_out, mlp_in, mlp_out,
    )
    return (grid_out, hidden_two)


def solution(mesh):
    part = P(("groups", "nodes"), None)
    nodes = P("nodes", None)
    return jax.shard_map(
        step,
        mesh=mesh,
        in_specs=(part, part, nodes, nodes) + (P(),) * 8,
        out_specs=(part, part),
        check_vma=False,
    )
```

```python
import jax
import jax.numpy as jnp
from jax import lax
from jax.experimental import pallas as pl
from jax.experimental.pallas import tpu as pltpu
from jax.sharding import PartitionSpec as P

HEADS = 16
LANES = 128
ONES = 16
CHUNK = 256
DEPTH = 2
EPSILON = 1e-05
LOG2E = 1.4426950408889634
MASKED = -1e30
TINY = 2.0**-100
HUGE = 2.0**100
BF16 = jnp.bfloat16
F32 = jnp.float32


def layer_norm(values):
    values = values.astype(F32)
    center = values - jnp.mean(values, axis=-1, keepdims=True)
    spread = jnp.mean(center * center, axis=-1, keepdims=True)
    return (center * lax.rsqrt(spread + EPSILON)).astype(BF16)


def dot(left, right):
    return jnp.dot(left, right, preferred_element_type=F32)


def dot_nt(left, right):
    return lax.dot_general(left, right, (((1,), (1,)), ((), ())), preferred_element_type=F32)


def block_columns(lists, pos, odd, rows):
    local = lists - pos * rows
    block = jnp.where(local < 0, -1, jnp.where(local < rows, 0, 1))
    inside = local - block * rows
    block = jnp.where(odd == 1, -block, block)
    return inside + jnp.where(block < 0, 2, block) * rows


def keep_values(kept, values, first):
    head_size = values.shape[1] // HEADS
    count = values.shape[0]
    turned = values.T
    for h in range(HEADS):
        kept[h, :head_size, first : first + count] = turned[h * head_size : (h + 1) * head_size]
        kept[h, head_size:, first : first + count] = jnp.ones((ONES, count), BF16)


def attend(q_ref, k_ref, kept, mix, counts_ref=None):
    width = k_ref.shape[1]
    head_size = width // HEADS
    keys = k_ref.shape[0]
    chunks = [slice(c, min(c + CHUNK, keys)) for c in range(0, keys, CHUNK)]
    least = largest = None
    waiting = []
    for head in range(HEADS + DEPTH):
        scores, mixed = [], None
        tile = head * head_size // LANES * LANES
        ready = waiting.pop(0) if head >= DEPTH else None
        for i, chunk in enumerate(chunks):
            if head < HEADS:
                scores.append(dot(k_ref[chunk, tile : tile + LANES], q_ref[head]))
            if ready is not None:
                weights = jnp.exp2(ready[i]).astype(BF16)
                if counts_ref is not None:
                    weights = weights * counts_ref[chunk]
                part = dot(kept[head - DEPTH, :, chunk], weights)
                mixed = part if mixed is None else mixed + part
        if head < HEADS:
            waiting.append(scores)
        if ready is not None:
            total = mixed[head_size : head_size + 1]
            first = (head - DEPTH) * head_size
            mix[first : first + head_size] = (mixed[:head_size] / total).astype(BF16)
            least = total if least is None else jnp.minimum(least, total)
            largest = total if largest is None else jnp.maximum(largest, total)
    return jnp.min(least), jnp.max(largest)


def attend_exactly(q_ref, k_ref, kept, mix, counts_ref=None):
    head_size = k_ref.shape[1] // HEADS

    def one_head(head, carry):
        tile = pl.multiple_of(head * head_size // LANES * LANES, LANES)
        scores = dot(k_ref[:, pl.ds(tile, LANES)], q_ref[head])
        if counts_ref is not None:
            scores = jnp.where(counts_ref[...].astype(F32) > 0.0, scores, MASKED)
        weights = jnp.exp2(scores - jnp.max(scores, axis=0, keepdims=True)).astype(BF16)
        if counts_ref is not None:
            weights = weights * counts_ref[...]
        mixed = dot(kept[head], weights)
        first = pl.multiple_of(head * head_size, head_size)
        mix[pl.ds(first, head_size)] = (
            mixed[:head_size] / mixed[head_size : head_size + 1]
        ).astype(BF16)
        return carry

    lax.fori_loop(0, HEADS, one_head, 0)


def attend_and_add(q_ref, k_ref, kept, mix, base_ref, out_ref, result_ref, counts_ref=None):
    def finish():
        added = dot(mix[...].T, out_ref[...])
        result_ref[...] = (base_ref[...].astype(F32) + added).astype(BF16)

    least, largest = attend(q_ref, k_ref, kept, mix, counts_ref)
    finish()

    @pl.when(jnp.logical_not(jnp.logical_and(least >= TINY, largest <= HUGE)))
    def _():
        attend_exactly(q_ref, k_ref, kept, mix, counts_ref)
        finish()


def spread_queries(target, queries):
    head_size = queries.shape[1] // HEADS
    turned = queries.T
    for head in range(HEADS):
        inside = head * head_size % LANES
        target[head] = jnp.zeros(target.shape[1:], BF16)
        target[head, inside : inside + head_size] = turned[head * head_size : (head + 1) * head_size]


def prepare_kernel(
    pos_ref, grid_hbm, hidden_hbm, enc_nbr_hbm, enc_qkv_hbm,
    queries_ref, pairs_ref, counts_ref,
    grid_ref, hidden_ref, enc_nbr_ref, enc_qkv_ref, arrived,
):
    width = grid_ref.shape[1]
    rows = grid_ref.shape[0]
    scale = LOG2E / (width // HEADS) ** 0.5
    copies = [
        pltpu.make_async_copy(source, target, arrived.at[i])
        for i, (source, target) in enumerate(
            [
                (enc_nbr_hbm, enc_nbr_ref),
                (grid_hbm, grid_ref),
                (hidden_hbm, hidden_ref),
                (enc_qkv_hbm, enc_qkv_ref),
            ]
        )
    ]
    for copy in copies:
        copy.start()
    copies[1].wait()
    copies[2].wait()
    normed = layer_norm(grid_ref[...])
    normed_hidden = layer_norm(hidden_ref[...])
    copies[3].wait()
    copies[0].wait()
    pairs_ref[...] = dot(normed, enc_qkv_ref[:, width:]).astype(BF16)
    queries = dot(normed_hidden, enc_qkv_ref[:, :width])
    spread_queries(queries_ref, (queries * scale).astype(BF16))
    pos = pos_ref[0]
    columns = block_columns(enc_nbr_ref[...], pos, pos % 2, rows)
    half = counts_ref.shape[0] // 2
    columns = (columns - half).astype(F32).astype(BF16)
    one = jnp.ones((rows, columns.shape[1]), BF16)
    for b in range(counts_ref.shape[0] // rows):
        places = b * rows - half + lax.broadcasted_iota(jnp.int32, one.shape, 0)
        places = places.astype(F32).astype(BF16)
        counts = jnp.zeros_like(one)
        for k in range(columns.shape[0]):
            counts = counts + jnp.where(columns[k : k + 1] == places, one, jnp.zeros_like(one))
        counts_ref[b * rows : (b + 1) * rows] = counts


def encode_kernel(
    queries_ref, pairs_ref, counts_ref, partner_ref, off_ref, hidden_ref, qkv_ref, out_ref,
    result_ref, keys, kept, mix,
):
    width = hidden_ref.shape[1]
    rows = pairs_ref.shape[0]
    keys[:rows] = pairs_ref[:, :width]
    keep_values(kept, pairs_ref[:, width:], 0)
    normed = jnp.concatenate([layer_norm(partner_ref[...]), layer_norm(off_ref[...])], axis=0)
    pairs = dot(normed, qkv_ref[:, width:]).astype(BF16)
    keys[rows:] = pairs[:, :width]
    keep_values(kept, pairs[:, width:], rows)
    attend_and_add(queries_ref, keys, kept, mix, hidden_ref, out_ref, result_ref, counts_ref)


def project_kernel(hidden_ref, qkv_ref, queries_ref, pairs_ref):
    width = hidden_ref.shape[1]
    scale = LOG2E / (width // HEADS) ** 0.5
    normed = layer_norm(hidden_ref[...])
    spread_queries(queries_ref, (dot(normed, qkv_ref[:, :width]) * scale).astype(BF16))
    pairs_ref[...] = dot(normed, qkv_ref[:, width:]).astype(BF16)


def process_kernel(
    queries_ref, pairs_ref, hidden_ref, partner_ref, qkv_ref, out_ref, result_ref, keys, kept, mix
):
    width = hidden_ref.shape[1]
    rows = hidden_ref.shape[0]
    keys[:rows] = pairs_ref[:, :width]
    keep_values(kept, pairs_ref[:, width:], 0)
    pairs = dot(layer_norm(partner_ref[...]), qkv_ref[:, width:]).astype(BF16)
    keys[rows:] = pairs[:, :width]
    keep_values(kept, pairs[:, width:], rows)
    attend_and_add(queries_ref, keys, kept, mix, hidden_ref, out_ref, result_ref)


def picks_of(columns, first, rows):
    places = first + lax.broadcasted_iota(jnp.int32, (columns.shape[0], rows), 1)
    return jnp.concatenate(
        [
            jnp.where(columns[:, j : j + 1] == places, 1.0, 0.0).astype(BF16)
            for j in range(columns.shape[1])
        ],
        axis=0,
    )


def gather_kernel(
    pos_ref, own_ref, partner_ref, nbr_ref, grid_hbm, qkv_hbm,
    two_hbm, queries_ref, picked_ref, off_picks_ref, grid_ref,
    normed, qkv_ref, arrived, written,
):
    width = own_ref.shape[1]
    rows = own_ref.shape[0]
    grid_copy = pltpu.make_async_copy(grid_hbm, grid_ref, arrived.at[0])
    qkv_copy = pltpu.make_async_copy(qkv_hbm.at[:, :width], qkv_ref, arrived.at[1])
    copy = pltpu.make_async_copy(own_ref, two_hbm, written)
    grid_copy.start()
    qkv_copy.start()
    copy.start()
    pos = pos_ref[0]
    columns = block_columns(nbr_ref[...], pos, pos % 2, rows)
    off_picks_ref[...] = picks_of(columns, 2 * rows, rows)
    normed[:rows] = layer_norm(own_ref[...])
    normed[rows:] = layer_norm(partner_ref[...])
    picked_ref[...] = dot(picks_of(columns, 0, 2 * rows), normed[...]).astype(BF16)
    grid_copy.wait()
    qkv_copy.wait()
    queries_ref[...] = dot(layer_norm(grid_ref[...]), qkv_ref[...]).astype(BF16)
    copy.wait()


def decode_kernel(
    off_ref, off_picks_ref, picked_ref, queries_ref, grid_ref, qkv_ref, out_ref,
    mlp_in_ref, mlp_out_ref, result_ref,
):
    width = off_ref.shape[1]
    head_size = width // HEADS
    grid_rows = grid_ref.shape[0]
    slots = picked_ref.shape[0] // grid_rows
    scale = LOG2E / head_size**0.5
    rows_picked = picked_ref[...] + dot(off_picks_ref[...], layer_norm(off_ref[...])).astype(BF16)
    pairs = dot(rows_picked, qkv_ref[:, width:]).astype(BF16)
    feature = lax.broadcasted_iota(jnp.int32, (width, LANES), 0) // head_size
    heads = lax.broadcasted_iota(jnp.int32, (width, LANES), 1)
    gather_heads = jnp.where(feature == heads, 1.0, 0.0).astype(BF16)
    queries = queries_ref[...].astype(F32)
    scores = []
    for j in range(slots):
        keys = pairs[j * grid_rows : (j + 1) * grid_rows, :width].astype(F32)
        scores.append(dot((queries * keys).astype(BF16), gather_heads) * scale)
    maxima = scores[0]
    for j in range(1, slots):
        maxima = jnp.maximum(maxima, scores[j])
    weights = [jnp.exp2(s - maxima) for s in scores]
    total = weights[0]
    for j in range(1, slots):
        total = total + weights[j]
    mix = None
    for j in range(slots):
        spread = dot_nt((weights[j] / total).astype(BF16), gather_heads)
        part = spread * pairs[j * grid_rows : (j + 1) * grid_rows, width:].astype(F32)
        mix = part if mix is None else mix + part
    grid_one = (grid_ref[...].astype(F32) + dot(mix.astype(BF16), out_ref[...])).astype(BF16)
    inner = jax.nn.gelu(dot(layer_norm(grid_one), mlp_in_ref[...])).astype(BF16)
    result_ref[...] = (grid_one.astype(F32) + dot(inner, mlp_out_ref[...])).astype(BF16)


def call(kernel, outs, scratch, flops, limit, *args, scalars=0, anywhere=(), out_anywhere=()):
    vmem = pl.BlockSpec(memory_space=pltpu.VMEM)
    smem = pl.BlockSpec(memory_space=pltpu.SMEM)
    hbm = pl.BlockSpec(memory_space=pltpu.HBM)
    args = [
        pltpu.with_memory_space_constraint(x, pltpu.HBM) if i in anywhere else x
        for i, x in enumerate(args)
    ]
    return pl.pallas_call(
        kernel,
        out_shape=[jax.ShapeDtypeStruct(shape, kind) for shape, kind in outs],
        in_specs=[
            smem if i < scalars else hbm if i in anywhere else vmem for i in range(len(args))
        ],
        out_specs=[hbm if i in out_anywhere else vmem for i in range(len(outs))],
        scratch_shapes=scratch,
        cost_estimate=pl.CostEstimate(flops=flops, transcendentals=0, bytes_accessed=0),
        compiler_params=pltpu.CompilerParams(vmem_limit_bytes=limit << 20),
    )(*args)


def attention_scratch(keys, rows, width):
    return [
        pltpu.VMEM((keys, width), BF16),
        pltpu.VMEM((HEADS, width // HEADS + ONES, keys), BF16),
        pltpu.VMEM((width, rows), BF16),
    ]


def step(
    grid, hidden, enc_nbr, dec_nbr, enc_qkv, enc_out, proc_qkv, proc_out, dec_qkv, dec_out,
    mlp_in, mlp_out,
):
    grid_rows, width = grid.shape
    rows = hidden.shape[0]
    slots = dec_nbr.shape[1]
    devices = lax.axis_size("nodes")
    pos = lax.axis_index("nodes").astype(jnp.int32).reshape(1)
    inner_pairs = [(i, i ^ 1) for i in range(devices)]
    outer_pairs = [(i, i + 1) for i in range(1, devices - 1, 2)]
    outer_pairs = outer_pairs + [(j, i) for i, j in outer_pairs]

    def exchange(shard):
        off = lax.ppermute(shard, "nodes", outer_pairs)
        return lax.ppermute(shard, "nodes", inner_pairs), off

    grid_partner, grid_off = exchange(grid)
    queries, pairs, counts = call(
        prepare_kernel,
        [((HEADS, LANES, rows), BF16), ((grid_rows, 2 * width), BF16), ((3 * grid_rows, rows), BF16)],
        [
            pltpu.VMEM(grid.shape, BF16),
            pltpu.VMEM(hidden.shape, BF16),
            pltpu.VMEM(enc_nbr.shape[::-1], jnp.int32),
            pltpu.VMEM(enc_qkv.shape, BF16),
            pltpu.SemaphoreType.DMA((4,)),
        ],
        2_000_000_000,
        16,
        pos, grid, hidden, enc_nbr.T, enc_qkv,
        scalars=1,
        anywhere=(1, 2, 3, 4),
    )
    (hidden_one,) = call(
        encode_kernel,
        [((rows, width), BF16)],
        attention_scratch(3 * grid_rows, rows, width),
        4_000_000_000,
        16,
        queries, pairs, counts, grid_partner, grid_off, hidden, enc_qkv, enc_out,
    )
    one_partner = lax.ppermute(hidden_one, "nodes", inner_pairs)
    queries, pairs = call(
        project_kernel,
        [((HEADS, LANES, rows), BF16), ((rows, 2 * width), BF16)],
        [],
        1_000_000_000,
        16,
        hidden_one, proc_qkv,
    )
    (two_near,) = call(
        process_kernel,
        [((rows, width), BF16)],
        attention_scratch(2 * rows, rows, width),
        4_000_000_000,
        16,
        queries, pairs, hidden_one, one_partner, proc_qkv, proc_out,
    )
    two_partner, two_off = exchange(two_near)
    hidden_two, dec_queries, picked, off_picks, grid_near = call(
        gather_kernel,
        [
            ((rows, width), BF16),
            ((grid_rows, width), BF16),
            ((slots * grid_rows, width), BF16),
            ((slots * grid_rows, rows), BF16),
            ((grid_rows, width), BF16),
        ],
        [
            pltpu.VMEM((2 * rows, width), BF16),
            pltpu.VMEM((width, width), BF16),
            pltpu.SemaphoreType.DMA((2,)),
            pltpu.SemaphoreType.DMA,
        ],
        1_000_000_000,
        16,
        pos, two_near, two_partner, dec_nbr, grid, dec_qkv,
        scalars=1,
        anywhere=(4, 5),
        out_anywhere=(0,),
    )
    (grid_out,) = call(
        decode_kernel,
        [((grid_rows, width), BF16)],
        [],
        4_000_000_000,
        16,
        two_off, off_picks, picked, dec_queries, grid_near, dec_qkv, dec_out, mlp_in, mlp_out,
    )
    return (grid_out, hidden_two)


def solution(mesh):
    part = P(("groups", "nodes"), None)
    nodes = P("nodes", None)
    return jax.shard_map(
        step,
        mesh=mesh,
        in_specs=(part, part, nodes, nodes) + (P(),) * 8,
        out_specs=(part, part),
        check_vma=False,
    )
```

```python
import functools

import jax
import jax.numpy as jnp
from jax import lax
from jax.experimental import pallas as pl
from jax.experimental.pallas import tpu as pltpu
from jax.sharding import PartitionSpec as P

HEADS = 16
LANES = 128
ONES = 16
CHUNK = 256
DEPTH = 2
EPSILON = 1e-05
LOG2E = 1.4426950408889634
MASKED = -1e30
TINY = 2.0**-100
HUGE = 2.0**100
BF16 = jnp.bfloat16
F32 = jnp.float32


def layer_norm(values):
    values = values.astype(F32)
    center = values - jnp.mean(values, axis=-1, keepdims=True)
    spread = jnp.mean(center * center, axis=-1, keepdims=True)
    return (center * lax.rsqrt(spread + EPSILON)).astype(BF16)


def dot(left, right):
    return jnp.dot(left, right, preferred_element_type=F32)


def dot_nt(left, right):
    return lax.dot_general(left, right, (((1,), (1,)), ((), ())), preferred_element_type=F32)


def block_columns(lists, pos, odd, rows):
    local = lists - pos * rows
    block = jnp.where(local < 0, -1, jnp.where(local < rows, 0, 1))
    inside = local - block * rows
    block = jnp.where(odd == 1, -block, block)
    return inside + jnp.where(block < 0, 2, block) * rows


def keep_values(kept, values, first):
    head_size = values.shape[1] // HEADS
    count = values.shape[0]
    turned = values.T
    for h in range(HEADS):
        kept[h, :head_size, first : first + count] = turned[h * head_size : (h + 1) * head_size]
        kept[h, head_size:, first : first + count] = jnp.ones((ONES, count), BF16)


def weigh(q_ref, k_ref, kept, consume, counts_ref=None):
    width = k_ref.shape[1]
    head_size = width // HEADS
    keys = k_ref.shape[0]
    chunks = [slice(c, min(c + CHUNK, keys)) for c in range(0, keys, CHUNK)]
    waiting = []
    for head in range(HEADS + DEPTH):
        scores, mixed = [], None
        tile = head * head_size // LANES * LANES
        ready = waiting.pop(0) if head >= DEPTH else None
        for i, chunk in enumerate(chunks):
            if head < HEADS:
                scores.append(dot(k_ref[chunk, tile : tile + LANES], q_ref[head]))
            if ready is not None:
                weights = jnp.exp2(ready[i]).astype(BF16)
                if counts_ref is not None:
                    weights = weights * counts_ref[chunk]
                part = dot(kept[head - DEPTH, :, chunk], weights)
                mixed = part if mixed is None else mixed + part
        if head < HEADS:
            waiting.append(scores)
        if ready is not None:
            consume(head - DEPTH, mixed)


def attend_exactly(q_ref, k_ref, kept, mix, counts_ref=None):
    head_size = k_ref.shape[1] // HEADS

    def one_head(head, carry):
        tile = pl.multiple_of(head * head_size // LANES * LANES, LANES)
        scores = dot(k_ref[:, pl.ds(tile, LANES)], q_ref[head])
        if counts_ref is not None:
            scores = jnp.where(counts_ref[...].astype(F32) > 0.0, scores, MASKED)
        weights = jnp.exp2(scores - jnp.max(scores, axis=0, keepdims=True)).astype(BF16)
        if counts_ref is not None:
            weights = weights * counts_ref[...]
        mixed = dot(kept[head], weights)
        first = pl.multiple_of(head * head_size, head_size)
        mix[pl.ds(first, head_size)] = (
            mixed[:head_size] / mixed[head_size : head_size + 1]
        ).astype(BF16)
        return carry

    lax.fori_loop(0, HEADS, one_head, 0)


def attend_and_add(
    q_ref, k_ref, kept, mix, base_ref, out_ref, result_ref, exactly, counts_ref=None, sums_ref=None
):
    head_size = k_ref.shape[1] // HEADS
    totals = []

    def consume(head, mixed):
        if sums_ref is not None:
            mixed = mixed + sums_ref[head]
        total = mixed[head_size : head_size + 1]
        totals.append(total)
        mix[head * head_size : (head + 1) * head_size] = (mixed[:head_size] / total).astype(BF16)

    def finish():
        added = dot(mix[...].T, out_ref[...])
        result_ref[...] = (base_ref[...].astype(F32) + added).astype(BF16)

    weigh(q_ref, k_ref, kept, consume, counts_ref)
    least = largest = totals[0]
    for total in totals[1:]:
        least, largest = jnp.minimum(least, total), jnp.maximum(largest, total)
    least, largest = jnp.min(least), jnp.max(largest)
    finish()

    @pl.when(jnp.logical_not(jnp.logical_and(least >= TINY, largest <= HUGE)))
    def _():
        exactly()
        finish()


def clear_queries(target):
    for head in range(HEADS):
        target[head] = jnp.zeros(target.shape[1:], BF16)


def spread_queries(target, queries):
    head_size = queries.shape[1] // HEADS
    turned = queries.T
    for head in range(HEADS):
        inside = head * head_size % LANES
        target[head, inside : inside + head_size] = turned[head * head_size : (head + 1) * head_size]


def prepare_kernel(
    pos_ref, grid_hbm, hidden_hbm, enc_nbr_hbm, enc_qkv_hbm,
    queries_ref, pairs_ref, counts_ref, hidden_ref, pair_weights,
    grid_ref, enc_nbr_ref, query_weights, arrived,
):
    width = grid_ref.shape[1]
    rows = grid_ref.shape[0]
    scale = LOG2E / (width // HEADS) ** 0.5
    copies = [
        pltpu.make_async_copy(source, target, arrived.at[i])
        for i, (source, target) in enumerate(
            [
                (enc_nbr_hbm, enc_nbr_ref),
                (hidden_hbm, hidden_ref),
                (grid_hbm, grid_ref),
                (enc_qkv_hbm.at[:, :width], query_weights),
                (enc_qkv_hbm.at[:, width:], pair_weights),
            ]
        )
    ]
    for copy in copies:
        copy.start()
    clear_queries(queries_ref)
    copies[0].wait()
    pos = pos_ref[0]
    columns = block_columns(enc_nbr_ref[...], pos, pos % 2, rows)
    half = counts_ref.shape[0] // 2
    columns = (columns - half).astype(F32).astype(BF16)
    one = jnp.ones((rows, columns.shape[1]), BF16)
    for b in range(counts_ref.shape[0] // rows):
        places = b * rows - half + lax.broadcasted_iota(jnp.int32, one.shape, 0)
        places = places.astype(F32).astype(BF16)
        counts = jnp.zeros_like(one)
        for k in range(columns.shape[0]):
            counts = counts + jnp.where(columns[k : k + 1] == places, one, jnp.zeros_like(one))
        counts_ref[b * rows : (b + 1) * rows] = counts
    for copy in copies[1:]:
        copy.wait()
    queries = dot(layer_norm(hidden_ref[...]), query_weights[...])
    spread_queries(queries_ref, (queries * scale).astype(BF16))
    pairs_ref[...] = dot(layer_norm(grid_ref[...]), pair_weights[...]).astype(BF16)


def encode_kernel(
    queries_ref, pairs_ref, counts_ref, partner_ref, off_ref, hidden_ref, pair_weights, out_ref,
    result_ref, keys, kept, mix,
):
    width = hidden_ref.shape[1]
    rows = pairs_ref.shape[0]
    keys[:rows] = pairs_ref[:, :width]
    keep_values(kept, pairs_ref[:, width:], 0)
    normed = jnp.concatenate([layer_norm(partner_ref[...]), layer_norm(off_ref[...])], axis=0)
    pairs = dot(normed, pair_weights[...]).astype(BF16)
    keys[rows:] = pairs[:, :width]
    keep_values(kept, pairs[:, width:], rows)
    exactly = functools.partial(attend_exactly, queries_ref, keys, kept, mix, counts_ref)
    attend_and_add(
        queries_ref, keys, kept, mix, hidden_ref, out_ref, result_ref, exactly, counts_ref
    )


def project_kernel(hidden_ref, qkv_ref, queries_ref, keys, kept, sums_ref):
    width = hidden_ref.shape[1]
    scale = LOG2E / (width // HEADS) ** 0.5
    clear_queries(queries_ref)
    normed = layer_norm(hidden_ref[...])
    spread_queries(queries_ref, (dot(normed, qkv_ref[:, :width]) * scale).astype(BF16))
    pairs = dot(normed, qkv_ref[:, width:]).astype(BF16)
    keys[...] = pairs[:, :width]
    keep_values(kept, pairs[:, width:], 0)

    def consume(head, mixed):
        sums_ref[head] = mixed

    weigh(queries_ref, keys, kept, consume)


def process_kernel(
    queries_ref, own_keys, own_kept, sums_ref, hidden_ref, partner_ref, qkv_ref, out_ref,
    result_ref, keys, kept, mix, all_keys, all_kept,
):
    width = hidden_ref.shape[1]
    rows = hidden_ref.shape[0]
    pairs = dot(layer_norm(partner_ref[...]), qkv_ref[:, width:]).astype(BF16)
    keys[...] = pairs[:, :width]
    keep_values(kept, pairs[:, width:], 0)

    def exactly():
        all_keys[:rows] = own_keys[...]
        all_keys[rows:] = keys[...]
        all_kept[:, :, :rows] = own_kept[...]
        all_kept[:, :, rows:] = kept[...]
        attend_exactly(queries_ref, all_keys, all_kept, mix)

    attend_and_add(
        queries_ref, keys, kept, mix, hidden_ref, out_ref, result_ref, exactly, sums_ref=sums_ref
    )


def picks_of(columns, first, rows):
    places = first + lax.broadcasted_iota(jnp.int32, (columns.shape[0], rows), 1)
    return jnp.concatenate(
        [
            jnp.where(columns[:, j : j + 1] == places, 1.0, 0.0).astype(BF16)
            for j in range(columns.shape[1])
        ],
        axis=0,
    )


def gather_kernel(
    pos_ref, own_ref, partner_ref, nbr_ref, grid_hbm, qkv_hbm,
    two_hbm, queries_ref, picked_ref, off_picks_ref, grid_ref,
    normed, qkv_ref, arrived, written,
):
    width = own_ref.shape[1]
    rows = own_ref.shape[0]
    grid_copy = pltpu.make_async_copy(grid_hbm, grid_ref, arrived.at[0])
    qkv_copy = pltpu.make_async_copy(qkv_hbm.at[:, :width], qkv_ref, arrived.at[1])
    copy = pltpu.make_async_copy(own_ref, two_hbm, written)
    grid_copy.start()
    qkv_copy.start()
    copy.start()
    pos = pos_ref[0]
    columns = block_columns(nbr_ref[...], pos, pos % 2, rows)
    off_picks_ref[...] = picks_of(columns, 2 * rows, rows)
    normed[:rows] = layer_norm(own_ref[...])
    normed[rows:] = layer_norm(partner_ref[...])
    picked_ref[...] = dot(picks_of(columns, 0, 2 * rows), normed[...]).astype(BF16)
    grid_copy.wait()
    qkv_copy.wait()
    queries_ref[...] = dot(layer_norm(grid_ref[...]), qkv_ref[...]).astype(BF16)
    copy.wait()


def decode_kernel(
    off_ref, off_picks_ref, picked_ref, queries_ref, grid_ref, qkv_ref, out_ref,
    mlp_in_ref, mlp_out_ref, result_ref,
):
    width = off_ref.shape[1]
    head_size = width // HEADS
    grid_rows = grid_ref.shape[0]
    slots = picked_ref.shape[0] // grid_rows
    scale = LOG2E / head_size**0.5
    rows_picked = picked_ref[...] + dot(off_picks_ref[...], layer_norm(off_ref[...])).astype(BF16)
    pairs = dot(rows_picked, qkv_ref[:, width:]).astype(BF16)
    feature = lax.broadcasted_iota(jnp.int32, (width, LANES), 0) // head_size
    heads = lax.broadcasted_iota(jnp.int32, (width, LANES), 1)
    gather_heads = jnp.where(feature == heads, 1.0, 0.0).astype(BF16)
    queries = queries_ref[...].astype(F32)
    scores = []
    for j in range(slots):
        keys = pairs[j * grid_rows : (j + 1) * grid_rows, :width].astype(F32)
        scores.append(dot((queries * keys).astype(BF16), gather_heads) * scale)
    maxima = scores[0]
    for j in range(1, slots):
        maxima = jnp.maximum(maxima, scores[j])
    weights = [jnp.exp2(s - maxima) for s in scores]
    total = weights[0]
    for j in range(1, slots):
        total = total + weights[j]
    mix = None
    for j in range(slots):
        spread = dot_nt((weights[j] / total).astype(BF16), gather_heads)
        part = spread * pairs[j * grid_rows : (j + 1) * grid_rows, width:].astype(F32)
        mix = part if mix is None else mix + part
    grid_one = (grid_ref[...].astype(F32) + dot(mix.astype(BF16), out_ref[...])).astype(BF16)
    inner = jax.nn.gelu(dot(layer_norm(grid_one), mlp_in_ref[...])).astype(BF16)
    result_ref[...] = (grid_one.astype(F32) + dot(inner, mlp_out_ref[...])).astype(BF16)


def call(kernel, outs, scratch, flops, limit, *args, scalars=0, anywhere=(), out_anywhere=()):
    vmem = pl.BlockSpec(memory_space=pltpu.VMEM)
    smem = pl.BlockSpec(memory_space=pltpu.SMEM)
    hbm = pl.BlockSpec(memory_space=pltpu.HBM)
    args = [
        pltpu.with_memory_space_constraint(x, pltpu.HBM) if i in anywhere else x
        for i, x in enumerate(args)
    ]
    return pl.pallas_call(
        kernel,
        out_shape=[jax.ShapeDtypeStruct(shape, kind) for shape, kind in outs],
        in_specs=[
            smem if i < scalars else hbm if i in anywhere else vmem for i in range(len(args))
        ],
        out_specs=[hbm if i in out_anywhere else vmem for i in range(len(outs))],
        scratch_shapes=scratch,
        cost_estimate=pl.CostEstimate(flops=flops, transcendentals=0, bytes_accessed=0),
        compiler_params=pltpu.CompilerParams(vmem_limit_bytes=limit << 20),
    )(*args)


def attention_scratch(keys, width):
    return [
        pltpu.VMEM((keys, width), BF16),
        pltpu.VMEM((HEADS, width // HEADS + ONES, keys), BF16),
    ]


def step(
    grid, hidden, enc_nbr, dec_nbr, enc_qkv, enc_out, proc_qkv, proc_out, dec_qkv, dec_out,
    mlp_in, mlp_out,
):
    grid_rows, width = grid.shape
    rows = hidden.shape[0]
    slots = dec_nbr.shape[1]
    devices = lax.axis_size("nodes")
    pos = lax.axis_index("nodes").astype(jnp.int32).reshape(1)
    inner_pairs = [(i, i ^ 1) for i in range(devices)]
    outer_pairs = [(i, i + 1) for i in range(1, devices - 1, 2)]
    outer_pairs = outer_pairs + [(j, i) for i, j in outer_pairs]

    def exchange(shard):
        off = lax.ppermute(shard, "nodes", outer_pairs)
        return lax.ppermute(shard, "nodes", inner_pairs), off

    grid_partner, grid_off = exchange(grid)
    kept_rows = width // HEADS + ONES
    queries, pairs, counts, hidden_near, pair_weights = call(
        prepare_kernel,
        [
            ((HEADS, LANES, rows), BF16),
            ((grid_rows, 2 * width), BF16),
            ((3 * grid_rows, rows), BF16),
            ((rows, width), BF16),
            ((width, 2 * width), BF16),
        ],
        [
            pltpu.VMEM(grid.shape, BF16),
            pltpu.VMEM(enc_nbr.shape[::-1], jnp.int32),
            pltpu.VMEM((width, width), BF16),
            pltpu.SemaphoreType.DMA((5,)),
        ],
        2_000_000_000,
        16,
        pos, grid, hidden, enc_nbr.T, enc_qkv,
        scalars=1,
        anywhere=(1, 2, 3, 4),
    )
    mix_scratch = pltpu.VMEM((width, rows), BF16)
    (hidden_one,) = call(
        encode_kernel,
        [((rows, width), BF16)],
        attention_scratch(3 * grid_rows, width) + [mix_scratch],
        4_000_000_000,
        16,
        queries, pairs, counts, grid_partner, grid_off, hidden_near, pair_weights, enc_out,
    )
    one_partner = lax.ppermute(hidden_one, "nodes", inner_pairs)
    queries, own_keys, own_kept, sums = call(
        project_kernel,
        [
            ((HEADS, LANES, rows), BF16),
            ((rows, width), BF16),
            ((HEADS, kept_rows, rows), BF16),
            ((HEADS, kept_rows, rows), F32),
        ],
        [],
        1_000_000_000,
        16,
        hidden_one, proc_qkv,
    )
    (two_near,) = call(
        process_kernel,
        [((rows, width), BF16)],
        attention_scratch(rows, width) + [mix_scratch] + attention_scratch(2 * rows, width),
        4_000_000_000,
        16,
        queries, own_keys, own_kept, sums, hidden_one, one_partner, proc_qkv, proc_out,
    )
    two_partner, two_off = exchange(two_near)
    hidden_two, dec_queries, picked, off_picks, grid_near = call(
        gather_kernel,
        [
            ((rows, width), BF16),
            ((grid_rows, width), BF16),
            ((slots * grid_rows, width), BF16),
            ((slots * grid_rows, rows), BF16),
            ((grid_rows, width), BF16),
        ],
        [
            pltpu.VMEM((2 * rows, width), BF16),
            pltpu.VMEM((width, width), BF16),
            pltpu.SemaphoreType.DMA((2,)),
            pltpu.SemaphoreType.DMA,
        ],
        1_000_000_000,
        16,
        pos, two_near, two_partner, dec_nbr, grid, dec_qkv,
        scalars=1,
        anywhere=(4, 5),
        out_anywhere=(0,),
    )
    (grid_out,) = call(
        decode_kernel,
        [((grid_rows, width), BF16)],
        [],
        4_000_000_000,
        16,
        two_off, off_picks, picked, dec_queries, grid_near, dec_qkv, dec_out, mlp_in, mlp_out,
    )
    return (grid_out, hidden_two)


def solution(mesh):
    part = P(("groups", "nodes"), None)
    nodes = P("nodes", None)
    return jax.shard_map(
        step,
        mesh=mesh,
        in_specs=(part, part, nodes, nodes) + (P(),) * 8,
        out_specs=(part, part),
        check_vma=False,
    )
```

```python
import jax
import jax.numpy as jnp
from jax import lax
from jax.experimental import pallas as pl
from jax.experimental.pallas import tpu as pltpu
from jax.sharding import PartitionSpec as P

HEADS = 16
LANES = 128
ONES = 16
DEPTH = 2
EPSILON = 1e-05
LOG2E = 1.4426950408889634
MASKED = -1e30
TINY = 2.0**-100
HUGE = 2.0**100
BF16 = jnp.bfloat16
F32 = jnp.float32


def layer_norm(values):
    values = values.astype(F32)
    center = values - jnp.mean(values, axis=-1, keepdims=True)
    spread = jnp.mean(center * center, axis=-1, keepdims=True)
    return (center * lax.rsqrt(spread + EPSILON)).astype(BF16)


def dot(left, right):
    return jnp.dot(left, right, preferred_element_type=F32)


def dot_nt(left, right):
    return lax.dot_general(left, right, (((1,), (1,)), ((), ())), preferred_element_type=F32)


def block_columns(lists, pos, odd, rows):
    local = lists - pos * rows
    block = jnp.where(local < 0, -1, jnp.where(local < rows, 0, 1))
    inside = local - block * rows
    block = jnp.where(odd == 1, -block, block)
    return inside + jnp.where(block < 0, 2, block) * rows


def keep_values(kept, values):
    head_size = values.shape[1] // HEADS
    turned = values.T
    for h in range(HEADS):
        kept[h, :head_size] = turned[h * head_size : (h + 1) * head_size]
        kept[h, head_size:] = jnp.ones((ONES, values.shape[0]), BF16)


def weigh(q_ref, parts, consume):
    head_size = parts[0][0].shape[1] // HEADS
    waiting = []
    for head in range(HEADS + DEPTH):
        scores, mixed = [], None
        tile = head * head_size // LANES * LANES
        ready = waiting.pop(0) if head >= DEPTH else None
        for i, (keys, kept, counts) in enumerate(parts):
            if head < HEADS:
                scores.append(dot(keys[:, tile : tile + LANES], q_ref[head]))
            if ready is not None:
                weights = jnp.exp2(ready[i]).astype(BF16)
                if counts is not None:
                    weights = weights * counts[...]
                part = dot(kept[head - DEPTH], weights)
                mixed = part if mixed is None else mixed + part
        if head < HEADS:
            waiting.append(scores)
        if ready is not None:
            consume(head - DEPTH, mixed)


def attend_exactly(q_ref, k_ref, kept, mix, counts_ref=None):
    head_size = k_ref.shape[1] // HEADS

    def one_head(head, carry):
        tile = pl.multiple_of(head * head_size // LANES * LANES, LANES)
        scores = dot(k_ref[:, pl.ds(tile, LANES)], q_ref[head])
        if counts_ref is not None:
            scores = jnp.where(counts_ref[...].astype(F32) > 0.0, scores, MASKED)
        weights = jnp.exp2(scores - jnp.max(scores, axis=0, keepdims=True)).astype(BF16)
        if counts_ref is not None:
            weights = weights * counts_ref[...]
        mixed = dot(kept[head], weights)
        first = pl.multiple_of(head * head_size, head_size)
        mix[pl.ds(first, head_size)] = (
            mixed[:head_size] / mixed[head_size : head_size + 1]
        ).astype(BF16)
        return carry

    lax.fori_loop(0, HEADS, one_head, 0)


def attend_and_add(
    q_ref, own, far, mix, all_keys, all_kept, base_ref, out_ref, result_ref, counts_ref=None
):
    width = all_keys.shape[1]
    head_size = width // HEADS
    rows = own[0].shape[0]
    counts = [None, None]
    if counts_ref is not None:
        counts = [counts_ref.at[:rows], counts_ref.at[rows:]]
    totals = []

    def consume(head, mixed):
        total = mixed[head_size : head_size + 1]
        totals.append(total)
        mix[head * head_size : (head + 1) * head_size] = (mixed[:head_size] / total).astype(BF16)

    def finish():
        added = dot(mix[...].T, out_ref[...])
        result_ref[...] = (base_ref[...].astype(F32) + added).astype(BF16)

    weigh(q_ref, [(*own, counts[0]), (*far, counts[1])], consume)
    least = largest = totals[0]
    for total in totals[1:]:
        least, largest = jnp.minimum(least, total), jnp.maximum(largest, total)
    least, largest = jnp.min(least), jnp.max(largest)
    finish()

    @pl.when(jnp.logical_not(jnp.logical_and(least >= TINY, largest <= HUGE)))
    def _():
        all_keys[:rows] = own[0][...]
        all_keys[rows:] = far[0][...]
        all_kept[:, :, :rows] = own[1][...]
        all_kept[:, :, rows:] = far[1][...]
        attend_exactly(q_ref, all_keys, all_kept, mix, counts_ref)
        finish()


def clear_queries(target):
    for head in range(HEADS):
        target[head] = jnp.zeros(target.shape[1:], BF16)


def spread_queries(target, queries):
    head_size = queries.shape[1] // HEADS
    turned = queries.T
    for head in range(HEADS):
        inside = head * head_size % LANES
        target[head, inside : inside + head_size] = turned[head * head_size : (head + 1) * head_size]


def prepare_kernel(
    pos_ref, grid_hbm, hidden_hbm, enc_nbr_hbm, enc_qkv_hbm,
    queries_ref, keys, kept, counts_ref, hidden_ref, pair_weights,
    grid_ref, enc_nbr_ref, query_weights, arrived,
):
    width = grid_ref.shape[1]
    rows = grid_ref.shape[0]
    scale = LOG2E / (width // HEADS) ** 0.5
    copies = [
        pltpu.make_async_copy(source, target, arrived.at[i])
        for i, (source, target) in enumerate(
            [
                (enc_nbr_hbm, enc_nbr_ref),
                (hidden_hbm, hidden_ref),
                (grid_hbm, grid_ref),
                (enc_qkv_hbm.at[:, :width], query_weights),
                (enc_qkv_hbm.at[:, width:], pair_weights),
            ]
        )
    ]
    for copy in copies:
        copy.start()
    clear_queries(queries_ref)
    copies[0].wait()
    pos = pos_ref[0]
    columns = block_columns(enc_nbr_ref[...], pos, pos % 2, rows)
    half = counts_ref.shape[0] // 2
    columns = (columns - half).astype(F32).astype(BF16)
    one = jnp.ones((rows, columns.shape[1]), BF16)
    for b in range(counts_ref.shape[0] // rows):
        places = b * rows - half + lax.broadcasted_iota(jnp.int32, one.shape, 0)
        places = places.astype(F32).astype(BF16)
        counts = jnp.zeros_like(one)
        for k in range(columns.shape[0]):
            counts = counts + jnp.where(columns[k : k + 1] == places, one, jnp.zeros_like(one))
        counts_ref[b * rows : (b + 1) * rows] = counts
    for copy in copies[1:]:
        copy.wait()
    queries = dot(layer_norm(hidden_ref[...]), query_weights[...])
    spread_queries(queries_ref, (queries * scale).astype(BF16))
    pairs = dot(layer_norm(grid_ref[...]), pair_weights[...]).astype(BF16)
    keys[...] = pairs[:, :width]
    keep_values(kept, pairs[:, width:])


def encode_kernel(
    queries_ref, own_keys, own_kept, counts_ref, partner_ref, off_ref, hidden_ref, pair_weights,
    out_ref, result_ref, keys, kept, mix, all_keys, all_kept,
):
    width = hidden_ref.shape[1]
    normed = jnp.concatenate([layer_norm(partner_ref[...]), layer_norm(off_ref[...])], axis=0)
    pairs = dot(normed, pair_weights[...]).astype(BF16)
    keys[...] = pairs[:, :width]
    keep_values(kept, pairs[:, width:])
    attend_and_add(
        queries_ref, (own_keys, own_kept), (keys, kept), mix, all_keys, all_kept,
        hidden_ref, out_ref, result_ref, counts_ref,
    )


def project_kernel(hidden_ref, qkv_ref, queries_ref, keys, kept):
    width = hidden_ref.shape[1]
    scale = LOG2E / (width // HEADS) ** 0.5
    clear_queries(queries_ref)
    normed = layer_norm(hidden_ref[...])
    spread_queries(queries_ref, (dot(normed, qkv_ref[:, :width]) * scale).astype(BF16))
    pairs = dot(normed, qkv_ref[:, width:]).astype(BF16)
    keys[...] = pairs[:, :width]
    keep_values(kept, pairs[:, width:])


def process_kernel(
    queries_ref, own_keys, own_kept, hidden_ref, partner_ref, qkv_ref, out_ref,
    result_ref, keys, kept, mix, all_keys, all_kept,
):
    width = hidden_ref.shape[1]
    pairs = dot(layer_norm(partner_ref[...]), qkv_ref[:, width:]).astype(BF16)
    keys[...] = pairs[:, :width]
    keep_values(kept, pairs[:, width:])
    attend_and_add(
        queries_ref, (own_keys, own_kept), (keys, kept), mix, all_keys, all_kept,
        hidden_ref, out_ref, result_ref,
    )


def picks_of(columns, first, rows):
    places = first + lax.broadcasted_iota(jnp.int32, (columns.shape[0], rows), 1)
    return jnp.concatenate(
        [
            jnp.where(columns[:, j : j + 1] == places, 1.0, 0.0).astype(BF16)
            for j in range(columns.shape[1])
        ],
        axis=0,
    )


def gather_kernel(
    pos_ref, own_ref, partner_ref, nbr_ref, grid_hbm, qkv_hbm,
    two_hbm, queries_ref, picked_ref, off_picks_ref, grid_ref,
    normed, qkv_ref, arrived, written,
):
    width = own_ref.shape[1]
    rows = own_ref.shape[0]
    grid_copy = pltpu.make_async_copy(grid_hbm, grid_ref, arrived.at[0])
    qkv_copy = pltpu.make_async_copy(qkv_hbm.at[:, :width], qkv_ref, arrived.at[1])
    copy = pltpu.make_async_copy(own_ref, two_hbm, written)
    grid_copy.start()
    qkv_copy.start()
    copy.start()
    pos = pos_ref[0]
    columns = block_columns(nbr_ref[...], pos, pos % 2, rows)
    off_picks_ref[...] = picks_of(columns, 2 * rows, rows)
    normed[:rows] = layer_norm(own_ref[...])
    normed[rows:] = layer_norm(partner_ref[...])
    picked_ref[...] = dot(picks_of(columns, 0, 2 * rows), normed[...]).astype(BF16)
    grid_copy.wait()
    qkv_copy.wait()
    queries_ref[...] = dot(layer_norm(grid_ref[...]), qkv_ref[...]).astype(BF16)
    copy.wait()


def decode_kernel(
    off_ref, off_picks_ref, picked_ref, queries_ref, grid_ref, qkv_ref, out_ref,
    mlp_in_ref, mlp_out_ref, result_ref,
):
    width = off_ref.shape[1]
    head_size = width // HEADS
    grid_rows = grid_ref.shape[0]
    slots = picked_ref.shape[0] // grid_rows
    scale = LOG2E / head_size**0.5
    rows_picked = picked_ref[...] + dot(off_picks_ref[...], layer_norm(off_ref[...])).astype(BF16)
    pairs = dot(rows_picked, qkv_ref[:, width:]).astype(BF16)
    feature = lax.broadcasted_iota(jnp.int32, (width, LANES), 0) // head_size
    heads = lax.broadcasted_iota(jnp.int32, (width, LANES), 1)
    gather_heads = jnp.where(feature == heads, 1.0, 0.0).astype(BF16)
    queries = queries_ref[...].astype(F32)
    scores = []
    for j in range(slots):
        keys = pairs[j * grid_rows : (j + 1) * grid_rows, :width].astype(F32)
        scores.append(dot((queries * keys).astype(BF16), gather_heads) * scale)
    maxima = scores[0]
    for j in range(1, slots):
        maxima = jnp.maximum(maxima, scores[j])
    weights = [jnp.exp2(s - maxima) for s in scores]
    total = weights[0]
    for j in range(1, slots):
        total = total + weights[j]
    mix = None
    for j in range(slots):
        spread = dot_nt((weights[j] / total).astype(BF16), gather_heads)
        part = spread * pairs[j * grid_rows : (j + 1) * grid_rows, width:].astype(F32)
        mix = part if mix is None else mix + part
    grid_one = (grid_ref[...].astype(F32) + dot(mix.astype(BF16), out_ref[...])).astype(BF16)
    inner = jax.nn.gelu(dot(layer_norm(grid_one), mlp_in_ref[...])).astype(BF16)
    result_ref[...] = (grid_one.astype(F32) + dot(inner, mlp_out_ref[...])).astype(BF16)


def call(kernel, outs, scratch, flops, limit, *args, scalars=0, anywhere=(), out_anywhere=()):
    vmem = pl.BlockSpec(memory_space=pltpu.VMEM)
    smem = pl.BlockSpec(memory_space=pltpu.SMEM)
    hbm = pl.BlockSpec(memory_space=pltpu.HBM)
    args = [
        pltpu.with_memory_space_constraint(x, pltpu.HBM) if i in anywhere else x
        for i, x in enumerate(args)
    ]
    return pl.pallas_call(
        kernel,
        out_shape=[jax.ShapeDtypeStruct(shape, kind) for shape, kind in outs],
        in_specs=[
            smem if i < scalars else hbm if i in anywhere else vmem for i in range(len(args))
        ],
        out_specs=[hbm if i in out_anywhere else vmem for i in range(len(outs))],
        scratch_shapes=scratch,
        cost_estimate=pl.CostEstimate(flops=flops, transcendentals=0, bytes_accessed=0),
        compiler_params=pltpu.CompilerParams(vmem_limit_bytes=limit << 20),
    )(*args)


def attention_scratch(keys, width):
    return [
        pltpu.VMEM((keys, width), BF16),
        pltpu.VMEM((HEADS, width // HEADS + ONES, keys), BF16),
    ]


def step(
    grid, hidden, enc_nbr, dec_nbr, enc_qkv, enc_out, proc_qkv, proc_out, dec_qkv, dec_out,
    mlp_in, mlp_out,
):
    grid_rows, width = grid.shape
    rows = hidden.shape[0]
    slots = dec_nbr.shape[1]
    devices = lax.axis_size("nodes")
    pos = lax.axis_index("nodes").astype(jnp.int32).reshape(1)
    inner_pairs = [(i, i ^ 1) for i in range(devices)]
    outer_pairs = [(i, i + 1) for i in range(1, devices - 1, 2)]
    outer_pairs = outer_pairs + [(j, i) for i, j in outer_pairs]

    def exchange(shard):
        off = lax.ppermute(shard, "nodes", outer_pairs)
        return lax.ppermute(shard, "nodes", inner_pairs), off

    grid_partner, grid_off = exchange(grid)
    kept_rows = width // HEADS + ONES
    queries, own_keys, own_kept, counts, hidden_near, pair_weights = call(
        prepare_kernel,
        [
            ((HEADS, LANES, rows), BF16),
            ((grid_rows, width), BF16),
            ((HEADS, kept_rows, grid_rows), BF16),
            ((3 * grid_rows, rows), BF16),
            ((rows, width), BF16),
            ((width, 2 * width), BF16),
        ],
        [
            pltpu.VMEM(grid.shape, BF16),
            pltpu.VMEM(enc_nbr.shape[::-1], jnp.int32),
            pltpu.VMEM((width, width), BF16),
            pltpu.SemaphoreType.DMA((5,)),
        ],
        2_000_000_000,
        16,
        pos, grid, hidden, enc_nbr.T, enc_qkv,
        scalars=1,
        anywhere=(1, 2, 3, 4),
    )
    mix_scratch = pltpu.VMEM((width, rows), BF16)
    (hidden_one,) = call(
        encode_kernel,
        [((rows, width), BF16)],
        attention_scratch(2 * grid_rows, width)
        + [mix_scratch]
        + attention_scratch(3 * grid_rows, width),
        4_000_000_000,
        16,
        queries, own_keys, own_kept, counts, grid_partner, grid_off, hidden_near, pair_weights,
        enc_out,
    )
    one_partner = lax.ppermute(hidden_one, "nodes", inner_pairs)
    queries, own_keys, own_kept = call(
        project_kernel,
        [
            ((HEADS, LANES, rows), BF16),
            ((rows, width), BF16),
            ((HEADS, kept_rows, rows), BF16),
        ],
        [],
        1_000_000_000,
        16,
        hidden_one, proc_qkv,
    )
    (two_near,) = call(
        process_kernel,
        [((rows, width), BF16)],
        attention_scratch(rows, width) + [mix_scratch] + attention_scratch(2 * rows, width),
        4_000_000_000,
        16,
        queries, own_keys, own_kept, hidden_one, one_partner, proc_qkv, proc_out,
    )
    two_partner, two_off = exchange(two_near)
    hidden_two, dec_queries, picked, off_picks, grid_near = call(
        gather_kernel,
        [
            ((rows, width), BF16),
            ((grid_rows, width), BF16),
            ((slots * grid_rows, width), BF16),
            ((slots * grid_rows, rows), BF16),
            ((grid_rows, width), BF16),
        ],
        [
            pltpu.VMEM((2 * rows, width), BF16),
            pltpu.VMEM((width, width), BF16),
            pltpu.SemaphoreType.DMA((2,)),
            pltpu.SemaphoreType.DMA,
        ],
        1_000_000_000,
        16,
        pos, two_near, two_partner, dec_nbr, grid, dec_qkv,
        scalars=1,
        anywhere=(4, 5),
        out_anywhere=(0,),
    )
    (grid_out,) = call(
        decode_kernel,
        [((grid_rows, width), BF16)],
        [],
        4_000_000_000,
        16,
        two_off, off_picks, picked, dec_queries, grid_near, dec_qkv, dec_out, mlp_in, mlp_out,
    )
    return (grid_out, hidden_two)


def solution(mesh):
    part = P(("groups", "nodes"), None)
    nodes = P("nodes", None)
    return jax.shard_map(
        step,
        mesh=mesh,
        in_specs=(part, part, nodes, nodes) + (P(),) * 8,
        out_specs=(part, part),
        check_vma=False,
    )
```
